256 devices in a mesh: rows: 64 (over y, z, x_hi), mem: 4 (over x_lo, core).
Axes of the slice: x: 4 (x_hi: 2, x_lo: 2; x = x_hi * 2 + x_lo), y: 4, z: 8, core: 2. Of those that a mesh axis runs over, the one named last changes fastest.
Arguments:
- state: float32 [16384, 5120], P('rows', 'mem')
- member_level: int32 [5120], P('mem'), may hold values from 0 to 3, as said below
- level_weight: float32 [4], replicated, may hold values from 0.3 to 3
- obs_row: int32 [1024], replicated, may hold values from 0 to 16383
- state_coords: int32 [2, 16384], replicated, may hold values from 0 to 255, as said below
- weights: float32 [1024, 5120], P('rows', 'mem'), may hold values from -6 to 6
Outputs:
- increment: float32 [16384, 5120], P('rows', 'mem')
The draws below stay inside these ranges and needn't reach their ends.
Inputs may be any that keep to these rules, and one draw needn't show every extreme that they name: `member_level`: every one of the 4 levels holds at least 2 members. `state_coords`: the first coordinate of row i lies within 2 of i // 64.
All inputs are finite; a program needn't handle non-finite values.
Results may differ from the reference program's by a relative error of at most 0.000073.
Values sent between devices are 32-bit elements; how exact they have to be, the bound alone decides.
A program may use at most 64 MiB of HBM per device.

```python
import math
import jax
import jax.numpy as jnp
from jax import lax

LEVELS = 4
NS = 16384
M = 5120
NO = 1024
GX = 256
GY = 64
RADIUS = 256


def member_levels(key):
    inner = jax.random.fold_in(key, 11)
    first_key, second_key = jax.random.split(inner)
    base = jax.random.randint(first_key, (M,), 0, LEVELS)
    order = jax.random.permutation(second_key, M)
    forced = jnp.arange(2 * LEVELS, dtype=jnp.int32) % LEVELS
    return base.at[order[:2 * LEVELS]].set(forced)


def draw_member_level(key, part):
    return member_levels(key).astype(jnp.int32)


def draw_state(key, part):
    levels = member_levels(key)
    inner = jax.random.fold_in(key, 23)
    keys = jax.random.split(inner, 4)
    row_mean = 3.0 * jax.random.normal(keys[0], (NS, 1), jnp.float32)
    bias = jax.random.normal(keys[1], (NS, LEVELS), jnp.float32)
    spread = jnp.exp(jax.random.uniform(keys[2], (NS, 1), jnp.float32, jnp.log(0.3), jnp.log(3.0)))
    noise = jax.random.normal(keys[3], (NS, M), jnp.float32)
    return (row_mean + jnp.take(bias, levels, axis=1) + spread * noise).astype(jnp.float32)


def draw_state_coords(key, part):
    inner = jax.random.fold_in(key, 31)
    first_key, second_key = jax.random.split(inner)
    jitter = jax.random.randint(first_key, (NS,), -2, 3)
    first = jnp.clip(jnp.arange(NS, dtype=jnp.int32) // GY + jitter, 0, GX - 1)
    second = jax.random.randint(second_key, (NS,), 0, GY)
    return jnp.stack([first, second]).astype(jnp.int32)


def with_ends(drawn, stream_key, low, largest):
    spot = [jax.random.randint(jax.random.fold_in(stream_key, axis), (), 0, length) for axis, length in enumerate(drawn.shape)]
    main_axis = drawn.shape.index(max(drawn.shape))
    neighbour = spot[:main_axis] + [(spot[main_axis] + 1) % drawn.shape[main_axis]] + spot[main_axis + 1:]
    return drawn.at[tuple(spot)].set(low).at[tuple(neighbour)].set(largest)


def block_scale(key, shape, shards, low, high):
    loudness = 1.0
    for dim, parts in shards:
        draws = jax.random.uniform(jax.random.fold_in(jax.random.fold_in(key, 6), dim), (parts,), jnp.float32, low / len(shards), high / len(shards))
        loudness = loudness * jnp.repeat(jnp.exp(draws), shape[dim] // parts).reshape((-1,) + (1,) * (len(shape) - 1 - dim))
    return loudness


def scatter_about(own_key, dims, width, most, pieces=(), kind=jnp.bfloat16):
    gain = block_scale(own_key, dims, pieces, -0.22, 0.18) if pieces else 1.0
    array = jax.random.normal(own_key, dims, jnp.float32) * width * gain
    return jnp.minimum(jnp.maximum(array, -most), most).astype(kind)


def setup_inputs(seed: int = 0) -> dict:
    key_list = jax.random.split(jax.random.key(seed), 7)
    state = draw_state(jax.random.fold_in(key_list[6], 71), 0)
    member_level = draw_member_level(jax.random.fold_in(key_list[6], 71), 0)
    level_weight = jnp.clip(jnp.exp(jax.random.uniform(key_list[2], (LEVELS,), jnp.float32, math.log(0.3), math.log(3.0))), 0.3, 3.0)
    obs_row = with_ends(jax.random.randint(key_list[3], (NO,), 0, NS), jax.random.fold_in(key_list[3], 1), 0, NS - 1).astype(jnp.int32)
    state_coords = draw_state_coords(jax.random.fold_in(key_list[6], 71), 0)
    weights = scatter_about(key_list[5], (NO, M), 1.0, 6.0, ((0, 64), (1, 4)), jnp.float32)
    return dict(state=state, member_level=member_level, level_weight=level_weight, obs_row=obs_row, state_coords=state_coords, weights=weights)


def reference(state, member_level, level_weight, obs_row, state_coords, weights):
    highest = lax.Precision.HIGHEST
    onehot = (member_level[:, None] == jnp.arange(LEVELS, dtype=jnp.int32)[None, :]).astype(jnp.float32)
    counts = jnp.sum(onehot, axis=0)
    sums = jnp.dot(state, onehot, precision=highest, preferred_element_type=jnp.float32)
    means = sums / counts[None, :]
    anomaly = state - jnp.take(means, member_level, axis=1)
    level_scale = level_weight / (counts - 1.0)
    scaled = anomaly * jnp.take(level_scale, member_level)[None, :]
    observed = jnp.take(anomaly, obs_row, axis=0)
    cross = jnp.dot(scaled, observed.T, precision=highest, preferred_element_type=jnp.float32)
    observed_xy = jnp.take(state_coords, obs_row, axis=1)
    offset_x = state_coords[0][:, None] - observed_xy[0][None, :]
    offset_y = state_coords[1][:, None] - observed_xy[1][None, :]
    distance = offset_x * offset_x + offset_y * offset_y
    reach = jnp.maximum(0.0, 1.0 - distance.astype(jnp.float32) / float(RADIUS * RADIUS))
    tapered = cross * (reach * reach)
    return jnp.dot(tapered, weights, precision=highest, preferred_element_type=jnp.float32)
```

```python
import functools

import jax
import jax.numpy as jnp
from jax import lax
from jax.experimental import pallas as pl
from jax.experimental.pallas import tpu as pltpu
from jax.sharding import PartitionSpec as P

MESH = pl.DeviceIdType.MESH
LEVELS = 4
NX, NY, NZ = 4, 4, 8
RADIUS = 256
F32 = jnp.float32
BF16 = jnp.bfloat16
NT = (((1,), (1,)), ((), ()))
NN = (((1,), (0,)), ((), ()))
COPIES = 192


def split(value):
    high = value.astype(BF16)
    return high, (value - high.astype(F32)).astype(BF16)


def dot(a, b, dims=NN):
    return lax.dot_general(a, b, dims, preferred_element_type=F32)


def dot3(a, b, dims=NN):
    return dot(a[0], b[0], dims) + dot(a[0], b[1], dims) + dot(a[1], b[0], dims)


def turns(chains):
    chains = list(chains)
    while chains:
        left = []
        for chain in chains:
            try:
                next(chain)
                left.append(chain)
            except StopIteration:
                pass
        chains = left
        if chains:
            yield


def in_turn(*parts):
    for part in parts:
        yield from part()


def drain(chain):
    for _ in chain:
        pass


def advance(chain, count):
    for _ in range(count):
        next(chain, None)


def kernel(
    state, level_all, level_kept, level_weight, obs_col, obs_row, table, row_xy, w_in,
    out,
    sums, kept, relay, s_high, s_low, pick_a, pick_b, got_az, got_ay, got_by, got_bz,
    seen_a, seen_b, w_a, w_b, cross, cross_in, got_x, t_all, send_sem, recv_sem,
):
    rows, mem = lax.axis_index("rows"), lax.axis_index("mem")
    y, z, xh = rows // (NZ * 2), (rows // 2) % NZ, rows % 2
    xl, core = mem // 2, mem % 2
    x = xh * 2 + xl
    count = [0]
    sent = []

    def at_y(k):
        return ((k * NZ + z) * 2 + xh, mem)

    def at_z(k):
        return ((y * NZ + k) * 2 + xh, mem)

    def at_x(k, c):
        return ((y * NZ + z) * 2 + k // 2, (k % 2) * 2 + c)

    def put(src, dst, device, landing=None):
        number = count[0]
        count[0] += 1
        out_copy = pltpu.make_async_remote_copy(
            src_ref=src, dst_ref=dst, send_sem=send_sem.at[number], recv_sem=recv_sem.at[number],
            device_id=device, device_id_type=MESH)
        out_copy.start()
        sent.append(out_copy)
        landing = dst if landing is None else landing
        return pltpu.make_async_remote_copy(
            src_ref=landing, dst_ref=landing, send_sem=send_sem.at[number],
            recv_sem=recv_sem.at[number], device_id=device, device_id_type=MESH)

    def gather_ring(n, p, block, device):
        def chain(way, half):
            hops = n // 2 if (half == 0) == (way == 1) else n // 2 - 1
            arriving = None
            for s in range(1, hops + 1):
                if arriving is not None:
                    arriving.wait_recv()
                out_block = block((p - way * (s - 1) + n) % n, half)
                in_block = block((p - way * s + n) % n, half)
                arriving = put(out_block, out_block, device((p + way + n) % n), in_block)
                yield
            if arriving is not None:
                arriving.wait_recv()
        return turns([chain(1, 0), chain(-1, 1), chain(1, 1), chain(-1, 0)])

    def scatter_ring(n, p, block, landing, device):
        def chain(way, half):
            hops = n // 2 if (half == 0) == (way == 1) else n // 2 - 1
            direction = 0 if way == 1 else 1
            arriving = None
            for s in range(1, hops + 1):
                part = block((p + way * (hops - s + 1) + n) % n, half)
                if arriving is not None:
                    arriving.wait_recv()
                    part[...] += landing[direction, half, s - 2]
                arriving = put(part, landing.at[direction, half, s - 1], device((p + way + n) % n))
                yield
            if arriving is not None:
                arriving.wait_recv()
                block(p, half)[...] += landing[direction, half, hops - 1]
        return turns([chain(1, 0), chain(-1, 1), chain(1, 1), chain(-1, 0)])

    def gather_plane(buf_a, buf_b):
        nb = buf_a.shape[2] // 2
        first = in_turn(
            lambda: gather_ring(NY, y, lambda k, h: buf_a.at[k, z, pl.ds(h * nb, nb)], at_y),
            lambda: gather_ring(NZ, z, lambda k, h: buf_a.at[pl.ds(h * (NY // 2), NY // 2), k], at_z))
        second = in_turn(
            lambda: gather_ring(NZ, z, lambda k, h: buf_b.at[y, k, pl.ds(h * nb, nb)], at_z),
            lambda: gather_ring(NY, y, lambda k, h: buf_b.at[k, pl.ds(h * (NZ // 2), NZ // 2)], at_y))
        return turns([second, first])

    def scatter_plane(buf_a, buf_b):
        nb = buf_a.shape[2] // 2
        first = in_turn(
            lambda: scatter_ring(NZ, z, lambda k, h: buf_a.at[pl.ds(h * (NY // 2), NY // 2), k], got_az, at_z),
            lambda: scatter_ring(NY, y, lambda k, h: buf_a.at[k, z, pl.ds(h * nb, nb)], got_ay, at_y))
        second = in_turn(
            lambda: scatter_ring(NY, y, lambda k, h: buf_b.at[k, pl.ds(h * (NZ // 2), NZ // 2)], got_by, at_y),
            lambda: scatter_ring(NZ, z, lambda k, h: buf_b.at[y, k, pl.ds(h * nb, nb)], got_bz, at_z))
        return turns([second, first])

    friends = [at_y((y + 1) % NY), at_y((y + NY - 1) % NY), at_z((z + 1) % NZ), at_z((z + NZ - 1) % NZ)]
    line = [at_x((x + d) % NX, c) for d in range(1, NX) for c in (core, 1 - core)]
    line.append(at_x(x, 1 - core))
    barrier = pltpu.get_barrier_semaphore()
    for device in friends + line:
        pl.semaphore_signal(barrier, inc=1, device_id=device, device_id_type=MESH)

    block_rows, members = state.shape
    half_members = members // 2
    level_ids = lax.broadcasted_iota(jnp.int32, (8, members), 0)
    own_level = level_all[...]
    onehot = (level_ids == own_level).astype(F32)
    counted = jnp.sum((level_ids - LEVELS == own_level).astype(F32), axis=1, keepdims=True)
    part = lax.dot_general(onehot, state[...], NT, precision=lax.Precision.HIGHEST, preferred_element_type=F32)
    sums[x * 2 + core] = part + counted

    depth, width_a = w_in.shape[0], w_a.shape[3]
    w_a[y, z, pl.ds(xh * depth, depth)] = w_in[:, :width_a]
    w_b[y, z, pl.ds(xh * depth, depth)] = w_in[:, width_a:]
    mine = pl.ds(pl.multiple_of(xh * half_members, 128), half_members)
    theirs = pl.ds(pl.multiple_of((1 - xh) * half_members, 128), half_members)
    kept[xh] = state[:, mine]

    pl.semaphore_wait(barrier, len(friends) + len(line))

    sums_in = []
    for d in range(1, NX):
        for c in (0, 1):
            device = at_x((x + d) % NX, (core + c) % 2)
            from_x, from_core = (x - d + NX) % NX, (core + c) % 2
            sums_in.append(put(sums.at[x * 2 + core], sums.at[x * 2 + core], device, sums.at[from_x * 2 + from_core]))
    sums_in.append(put(sums.at[x * 2 + core], sums.at[x * 2 + core], at_x(x, 1 - core), sums.at[x * 2 + 1 - core]))
    partner = at_x((x + 2) % NX, core)
    own_part, other_part = pl.ds(xh * depth, depth), pl.ds((1 - xh) * depth, depth)
    w_pair = [put(buf.at[y, z, own_part], buf.at[y, z, own_part], partner, buf.at[y, z, other_part]) for buf in (w_b, w_a)]
    piece = block_rows // 4
    first_hop = []
    for k in (0, 2, 1, 3):
        way = 1 if k < 2 else NX - 1
        first_hop.append((k, way, put(state.at[pl.ds(k * piece, piece), theirs], relay.at[k], at_x((x + way) % NX, core))))

    def relay_on(number):
        k, way, arriving = first_hop[number]
        arriving.wait_recv()
        origin = ((x - way + NX) % NX) // 2
        spot = pl.ds(k * piece, piece)
        return put(relay.at[k], kept.at[origin, spot], at_x((x + way) % NX, core), kept.at[1 - xh, spot])

    for arriving in w_pair:
        arriving.wait_recv()
    w_chain = gather_plane(w_a, w_b)
    advance(w_chain, 1)

    for arriving in sums_in:
        arriving.wait_recv()
    kept_level = level_kept[...]
    total = [sums[h * 4] + sums[h * 4 + 1] + sums[h * 4 + 2] + sums[h * 4 + 3] for h in (0, 1)]
    means = [(t / jnp.concatenate([t[LEVELS:], t[LEVELS:]], axis=0)).T for t in total]
    scale = jnp.zeros((1, half_members), F32)
    for l in range(LEVELS):
        value = level_weight[l] / (total[0][LEVELS + l : LEVELS + l + 1, 0:1] - 1.0)
        scale = jnp.where(kept_level == l, value, scale)
    block = rows // 2

    def prepare(h, first):
        mean = jnp.where(h == 0, means[0], means[1])
        shift = jnp.zeros((block_rows, half_members), F32)
        for l in range(LEVELS):
            shift = jnp.where(kept_level == l, mean[:, l : l + 1], shift)
        anomaly = kept[h] - shift
        high, low = split(anomaly * scale)
        s_high[h], s_low[h] = high, low
        high, low = split(anomaly)
        row_ids = lax.broadcasted_iota(jnp.int32, (NY * 64, block_rows), 1) + (block * 2 + h) * block_rows
        per = NY * 64
        for k in range(obs_col.shape[0] // per):
            chosen = (obs_col[pl.ds(k * per, per)] == row_ids).astype(BF16)
            picked = dot(chosen, high) + dot(chosen, low)
            a = picked[:, : pick_a.shape[3]].reshape(NZ, per // NZ, pick_a.shape[3])
            b = picked[:, pick_a.shape[3] :].reshape(NZ, per // NZ, pick_b.shape[3])
            pick_a[k] = a if first else pick_a[k] + a
            pick_b[k] = b if first else pick_b[k] + b

    final_hop = [relay_on(0), relay_on(1)]
    advance(w_chain, 1)
    prepare(xh, True)
    final_hop += [relay_on(2), relay_on(3)]
    advance(w_chain, 2)
    for arriving in final_hop:
        arriving.wait_recv()
    prepare(1 - xh, False)
    advance(w_chain, 1)

    drain(scatter_plane(pick_a, pick_b))
    advance(w_chain, 1)
    seen_a[y, z] = pick_a[y, z]
    seen_b[y, z] = pick_b[y, z]
    drain(gather_plane(seen_a, seen_b))
    advance(w_chain, 1)

    wide_a = seen_a.shape[3]
    s_a = [jnp.concatenate([ref[0, :, :wide_a], ref[1, :, :wide_a]], axis=0) for ref in (s_high, s_low)]
    s_b = [jnp.concatenate([ref[0, :, wide_a:], ref[1, :, wide_a:]], axis=0) for ref in (s_high, s_low)]
    per = NZ * seen_a.shape[2]
    for k in range(NY):
        o_a = split(seen_a[k].reshape(per, wide_a))
        o_b = split(seen_b[k].reshape(per, seen_b.shape[3]))
        c = dot3(s_a, o_a, NT) + dot3(s_b, o_b, NT)
        cross[:, :, :, k * per : (k + 1) * per] = c.reshape(NX, 2, c.shape[0] // (2 * NX), per).swapaxes(0, 1)

    pair = put(cross.at[1 - core], cross_in, at_x(x, 1 - core))
    pair.wait_recv()
    cross[core] += cross_in[...]
    rows_each = cross.shape[2]
    advance(w_chain, 1)
    drain(scatter_ring(NX, x, lambda k, h: cross.at[core, k, pl.ds(h * (rows_each // 2), rows_each // 2)], got_x,
                       lambda k: at_x(k, core)))
    advance(w_chain, 1)

    seen_rows = obs_row[...]
    high_ids = lax.broadcasted_iota(jnp.int32, (128, seen_rows.shape[1]), 0)
    is_high = (high_ids == seen_rows // 128).astype(BF16)
    is_low = high_ids == seen_rows % 128
    seen_x = jnp.sum(jnp.where(is_low, dot(table[0], is_high), 0.0), axis=0, keepdims=True)
    seen_y = jnp.sum(jnp.where(is_low, dot(table[1], is_high), 0.0), axis=0, keepdims=True)
    apart_x = row_xy[:, 0:1] - seen_x
    apart_y = row_xy[:, 1:2] - seen_y
    reach = jnp.maximum(0.0, 1.0 - (apart_x * apart_x + apart_y * apart_y) / float(RADIUS * RADIUS))
    t_all[mem] = cross[core, x] * (reach * reach)

    across = put(t_all.at[mem], t_all.at[mem], at_x(xh * 2 + 1 - xl, core), t_all.at[(1 - xl) * 2 + core])
    beside = put(t_all.at[mem], t_all.at[mem], at_x(x, 1 - core), t_all.at[xl * 2 + 1 - core])
    advance(w_chain, 1)
    across.wait_recv()
    there = (1 - xl) * 2
    passed = put(t_all.at[there + core], t_all.at[there + core], at_x(x, 1 - core), t_all.at[there + 1 - core])
    drain(w_chain)
    beside.wait_recv()
    passed.wait_recv()

    t = split(t_all[...].reshape(block_rows, t_all.shape[2]))
    step = 256
    for buf, start in ((w_a, 0), (w_b, width_a)):
        for k in range(buf.shape[3] // step):
            w = split(buf[:, :, :, k * step : (k + 1) * step].reshape(t_all.shape[2], step))
            out[:, start + k * step : start + (k + 1) * step] = dot3(t, w)

    for copy in sent:
        copy.wait_send()


def on_device(state, member_level, level_weight, obs_row, state_coords, weights):
    rows, mem = lax.axis_index("rows"), lax.axis_index("mem")
    block_rows, members = state.shape
    observations = obs_row.shape[0]
    half = members // 2
    kept = lax.dynamic_slice_in_dim(member_level, (rows % 2) * half, half)
    own = block_rows // 4
    row_xy = lax.dynamic_slice_in_dim(state_coords, rows * block_rows + mem * own, own, 1).T.astype(F32)
    table = state_coords.reshape(2, -1, 128).swapaxes(1, 2).astype(BF16)
    depth = weights.shape[0]
    per = 2 * depth
    a, b = half * 2 // 5, half * 3 // 5
    hy, hz = NY // 2, NZ // 2
    vmem = pl.BlockSpec(memory_space=pltpu.VMEM)
    smem = pl.BlockSpec(memory_space=pltpu.SMEM)
    return pl.pallas_call(
        kernel,
        out_shape=jax.ShapeDtypeStruct((block_rows, members), F32),
        in_specs=[vmem, vmem, vmem, smem, vmem, vmem, vmem, vmem, vmem],
        out_specs=vmem,
        scratch_shapes=[
            pltpu.VMEM((NX * 2, 8, block_rows), F32),
            pltpu.VMEM((2, block_rows, half), F32),
            pltpu.VMEM((4, block_rows // 4, half), F32),
            pltpu.VMEM((2, block_rows, half), BF16),
            pltpu.VMEM((2, block_rows, half), BF16),
            pltpu.VMEM((NY, NZ, per, a), F32),
            pltpu.VMEM((NY, NZ, per, b), F32),
            pltpu.VMEM((2, 2, hz, hy, per, a), F32),
            pltpu.VMEM((2, 2, hy, per // 2, a), F32),
            pltpu.VMEM((2, 2, hy, hz, per, b), F32),
            pltpu.VMEM((2, 2, hz, per // 2, b), F32),
            pltpu.VMEM((NY, NZ, per, a), F32),
            pltpu.VMEM((NY, NZ, per, b), F32),
            pltpu.VMEM((NY, NZ, per, members * 2 // 5), F32),
            pltpu.VMEM((NY, NZ, per, members * 3 // 5), F32),
            pltpu.VMEM((2, NX, own, observations), F32),
            pltpu.VMEM((NX, own, observations), F32),
            pltpu.VMEM((2, 2, 2, own // 2, observations), F32),
            pltpu.VMEM((4, own, observations), F32),
            pltpu.SemaphoreType.DMA((COPIES,)),
            pltpu.SemaphoreType.DMA((COPIES,)),
        ],
        compiler_params=pltpu.CompilerParams(
            collective_id=0, has_side_effects=True, vmem_limit_bytes=60 * 1024 * 1024),
    )(
        state, member_level.reshape(1, -1), kept.reshape(1, -1), level_weight,
        obs_row.reshape(-1, 1), obs_row.reshape(1, -1), table, row_xy, weights,
    )


def solution(mesh):
    return jax.shard_map(
        on_device,
        mesh=mesh,
        in_specs=(P("rows", "mem"), P("mem"), P(), P(), P(), P("rows", "mem")),
        out_specs=P("rows", "mem"),
        check_vma=False,
    )
```

```python
import math

import jax
import jax.numpy as jnp
from jax import lax
from jax.experimental import pallas as pl
from jax.experimental.pallas import tpu as pltpu
from jax.sharding import PartitionSpec as P

MESH = pl.DeviceIdType.MESH
LEVELS = 4
NX, NY, NZ = 4, 4, 8
RADIUS = 256
F32 = jnp.float32
BF16 = jnp.bfloat16
NT = (((1,), (1,)), ((), ()))
NN = (((1,), (0,)), ((), ()))
COPIES = 229
PIECES = 8
VMEM_BYTES = 67043328
SENDS = 16
STRAIGHT = 4


def split(value):
    high = value.astype(BF16)
    return high, (value - high.astype(F32)).astype(BF16)


def dot(a, b, dims=NN):
    return lax.dot_general(a, b, dims, preferred_element_type=F32)


def dot3(a, b, dims=NN):
    return dot(a[0], b[0], dims) + dot(a[0], b[1], dims) + dot(a[1], b[0], dims)


def turns(chains):
    chains = list(chains)
    while chains:
        left = []
        for chain in chains:
            try:
                next(chain)
                left.append(chain)
            except StopIteration:
                pass
        chains = left
        if chains:
            yield


def drain(chain):
    for _ in chain:
        pass


def advance(chain, count):
    for _ in range(count):
        next(chain, None)


def kernel(
    state_far, level_far, level_weight, obs_far, coords_far, w_far,
    out,
    state, level_line, obs_line, coords, w_in, table,
    sums, kept, relay, s_high, s_low, pick_a, pick_b, got_az, got_ay, got_by, got_bz,
    seen_a, seen_b, w_a, w_b, cross, cross_in, got_x, t_all, ledger, send_sem, recv_sem, straight_sem, load_sem,
):
    rows, mem = lax.axis_index("rows"), lax.axis_index("mem")
    y, z, xh = rows // (NZ * 2), (rows // 2) % NZ, rows % 2
    xl, core = mem // 2, mem % 2
    x = xh * 2 + xl
    count = [0]
    sent = []

    def at_y(k):
        return ((k * NZ + z) * 2 + xh, mem)

    def at_z(k):
        return ((y * NZ + k) * 2 + xh, mem)

    def at_x(k, c):
        return ((y * NZ + z) * 2 + k // 2, (k % 2) * 2 + c)

    def put(src, dst, device, landing=None, arrival=None):
        recv = recv_sem.at[count[0]]
        if arrival is None:
            arrival = recv
            count[0] += 1
        group = len(sent) % SENDS
        copy = pltpu.make_async_remote_copy(
            src_ref=src, dst_ref=dst, send_sem=send_sem.at[group], recv_sem=arrival,
            device_id=device, device_id_type=MESH)
        copy.start()
        sent.append(math.prod(src.shape) // 128)
        if arrival is not recv:
            return None
        landing = dst if landing is None else landing
        return pltpu.make_async_remote_copy(
            src_ref=landing, dst_ref=landing, send_sem=send_sem.at[group],
            recv_sem=arrival, device_id=device, device_id_type=MESH)

    def all_lines(lines, semaphore):
        whole = ledger.at[pl.ds(0, lines)]
        return pltpu.make_async_remote_copy(
            src_ref=whole, dst_ref=whole, send_sem=semaphore, recv_sem=semaphore,
            device_id=at_x(x, 1 - core), device_id_type=MESH)

    def gather_ring(n, p, block, device, only=None):
        def chain(way, half):
            hops = n // 2 if (half == 0) == (way == 1) else n // 2 - 1
            arriving = None
            for s in range(1, hops + 1):
                if arriving is not None:
                    arriving.wait_recv()
                out_block = block((p - way * (s - 1) + n) % n, half)
                in_block = block((p - way * s + n) % n, half)
                arriving = put(out_block, out_block, device((p + way + n) % n), in_block)
                yield
            if arriving is not None:
                arriving.wait_recv()
        order = [(1, 0), (-1, 1), (1, 1), (-1, 0)]
        return turns([chain(way, half) for way, half in order if only in (None, half)])

    def scatter_ring(n, p, block, landing, device):
        def chain(way, half):
            hops = n // 2 if (half == 0) == (way == 1) else n // 2 - 1
            direction = 0 if way == 1 else 1
            arriving = None
            for s in range(1, hops + 1):
                part = block((p + way * (hops - s + 1) + n) % n, half)
                if arriving is not None:
                    arriving.wait_recv()
                    part[...] += landing[direction, half, s - 2]
                arriving = put(part, landing.at[direction, half, s - 1], device((p + way + n) % n))
                yield
            if arriving is not None:
                arriving.wait_recv()
                block(p, half)[...] += landing[direction, half, hops - 1]
        return turns([chain(1, 0), chain(-1, 1), chain(1, 1), chain(-1, 0)])

    def far_first(n):
        return sorted(range(1, n), key=lambda d: abs(d - n // 2))

    def scatter_straight(n, p, block, landing, device, arrival):
        for d in far_first(n):
            q = (p + d) % n
            put(block(q), landing.at[d - 1], device(q), arrival=arrival)
        yield
        all_lines((n - 1) * math.prod(landing.shape[1:]) // 128, arrival).wait_recv()
        block(p)[...] += sum(landing[d - 1] for d in range(1, n))

    def gather_straight(n, p, block, device, arrival):
        for d in far_first(n):
            put(block(p), block(p), device((p + d) % n), arrival=arrival)
        yield
        all_lines((n - 1) * math.prod(block(p).shape) // 128, arrival).wait_recv()

    def gather_fine(n, p, outer, inner):
        going, done, r = [inner(p)], False, 0
        while going or not done:
            if not done:
                try:
                    next(outer)
                except StopIteration:
                    done = True
                if r > 0:
                    going.append(inner((p + r) % n))
                    if 2 * r < n:
                        going.append(inner((p - r + n) % n))
                r += 1
            left = []
            for chain in going:
                try:
                    next(chain)
                    left.append(chain)
                except StopIteration:
                    pass
            going = left
            yield

    def part(h):
        return pl.ds((h + xh) % 2 * w_in.shape[0], w_in.shape[0])

    def y_outer(buf, own):
        return gather_fine(
            NY, y, gather_ring(NY, y, lambda k, h: buf.at[k, z, part(h)], at_y, own),
            lambda j: gather_ring(NZ, z, lambda k, h: buf.at[j, k, part(h)], at_z, own))

    def z_outer(buf, own):
        return gather_fine(
            NZ, z, gather_ring(NZ, z, lambda k, h: buf.at[y, k, part(h)], at_z, own),
            lambda j: gather_ring(NY, y, lambda k, h: buf.at[k, j, part(h)], at_y, own))

    friends = [at_y((y + 1) % NY), at_y((y + NY - 1) % NY), at_z((z + 1) % NZ), at_z((z + NZ - 1) % NZ)]
    line = [at_x((x + d) % NX, c) for d in range(1, NX) for c in (core, 1 - core)]
    line.append(at_x(x, 1 - core))
    barrier = pltpu.get_barrier_semaphore()
    for device in friends + line:
        pl.semaphore_signal(barrier, inc=1, device_id=device, device_id_type=MESH)

    loads = [pltpu.make_async_copy(far, near, load_sem.at[n]) for n, (far, near) in enumerate((
        (w_far, w_in), (state_far, state), (level_far, level_line), (obs_far, obs_line), (coords_far, coords)))]
    for load in loads:
        load.start()
    block_rows, members = state.shape
    half_members = members // 2
    observations = obs_line.shape[0]
    loads[0].wait()
    depth, width_a = w_in.shape[0], w_a.shape[3]
    w_a[y, z, pl.ds(xh * depth, depth)] = w_in[:, :width_a]
    w_b[y, z, pl.ds(xh * depth, depth)] = w_in[:, width_a:]
    mine = pl.ds(pl.multiple_of(xh * half_members, 128), half_members)
    theirs = pl.ds(pl.multiple_of((1 - xh) * half_members, 128), half_members)

    for load in loads[1:]:
        load.wait()
    level_all = level_line[...].reshape(1, members)
    obs_all = obs_line[...].reshape(1, observations)
    pl.semaphore_wait(barrier, len(friends) + len(line))

    partner = at_x((x + 2) % NX, core)
    own_part, other_part = pl.ds(xh * depth, depth), pl.ds((1 - xh) * depth, depth)
    w_pair = [put(buf.at[y, z, own_part], buf.at[y, z, own_part], partner, buf.at[y, z, other_part]) for buf in (w_b, w_a)]
    piece = block_rows // PIECES
    hops = []
    for n in range(PIECES):
        k = n // 2 + (n % 2) * (PIECES // 2)
        way = 1 if n % 2 == 0 else NX - 1
        hops.append((k, way, put(state.at[pl.ds(k * piece, piece), theirs], relay.at[k], at_x((x + way) % NX, core))))

    def pass_on(numbers):
        landed = []
        for n in numbers:
            k, way, arriving = hops[n]
            arriving.wait_recv()
            origin = ((x - way + NX) % NX) // 2
            spot = pl.ds(k * piece, piece)
            landed.append(put(relay.at[k], kept.at[origin, spot], at_x((x + way) % NX, core), kept.at[1 - xh, spot]))
        return landed

    level_ids = lax.broadcasted_iota(jnp.int32, (8, members), 0)
    own_level = level_all
    onehot = (level_ids == own_level).astype(F32)
    counted = jnp.sum((level_ids - LEVELS == own_level).astype(F32), axis=1, keepdims=True)
    summed = lax.dot_general(onehot, state[...], NT, precision=lax.Precision.HIGHEST, preferred_element_type=F32)
    sums[x * 2 + core] = summed + counted
    sums_in = []
    for d in range(1, NX):
        for c in (0, 1):
            device = at_x((x + d) % NX, (core + c) % 2)
            from_x, from_core = (x - d + NX) % NX, (core + c) % 2
            sums_in.append(put(sums.at[x * 2 + core], sums.at[x * 2 + core], device, sums.at[from_x * 2 + from_core]))
    sums_in.append(put(sums.at[x * 2 + core], sums.at[x * 2 + core], at_x(x, 1 - core), sums.at[x * 2 + 1 - core]))
    kept[xh] = state[:, mine]
    kept_level = jnp.where(xh == 0, level_all[:, :half_members], level_all[:, half_members:])
    block = rows // 2
    obs_col = jnp.broadcast_to(obs_all, (8, observations)).T[:, 0:1]

    def move_weights():
        own = turns([z_outer(w_b, 0), y_outer(w_a, 0)])
        other = turns([z_outer(w_b, 1), y_outer(w_a, 1)])
        next(own)
        for arriving in w_pair:
            arriving.wait_recv()
        next(other)
        yield
        yield from turns([own, other])

    for k in range(table.shape[1]):
        table[:, k, :] = coords[:, k * 128 : (k + 1) * 128]

    w_chain = move_weights()
    advance(w_chain, 1)
    landed = pass_on(range(0, PIECES // 2))
    advance(w_chain, 1)
    landed += pass_on(range(PIECES // 2, PIECES))
    for arriving in sums_in:
        arriving.wait_recv()
    total = [sums[h * 4] + sums[h * 4 + 1] + sums[h * 4 + 2] + sums[h * 4 + 3] for h in (0, 1)]
    means = [(t / jnp.concatenate([t[LEVELS:], t[LEVELS:]], axis=0)).T for t in total]
    scale = jnp.zeros((1, half_members), F32)
    for l in range(LEVELS):
        value = level_weight[l] / (total[0][LEVELS + l : LEVELS + l + 1, 0:1] - 1.0)
        scale = jnp.where(kept_level == l, value, scale)

    wide_a = pick_a.shape[3]
    per = NZ * pick_a.shape[2]

    def prepare(h, first):
        mean = jnp.where(h == 0, means[0], means[1])
        shift = jnp.zeros((block_rows, half_members), F32)
        for l in range(LEVELS):
            shift = jnp.where(kept_level == l, mean[:, l : l + 1], shift)
        anomaly = kept[h] - shift
        s_high[h], s_low[h] = split(anomaly * scale)
        high, low = split(anomaly)
        row_ids = lax.broadcasted_iota(jnp.int32, (per, block_rows), 1) + (block * 2 + h) * block_rows
        for k in range(NY):
            chosen = (obs_col[k * per : (k + 1) * per] == row_ids).astype(BF16)
            picked = dot(chosen, high) + dot(chosen, low)
            a = picked[:, :wide_a].reshape(NZ, per // NZ, wide_a)
            b = picked[:, wide_a:].reshape(NZ, per // NZ, half_members - wide_a)
            pick_a[k] = a if first else pick_a[k] + a
            pick_b[k] = b if first else pick_b[k] + b

    prepare(xh, True)
    advance(w_chain, 1)
    for arriving in landed:
        arriving.wait_recv()
    prepare(1 - xh, False)

    nb = pick_a.shape[2] // 2
    hy, hz = NY // 2, NZ // 2
    a_chain = scatter_ring(NZ, z, lambda k, h: pick_a.at[pl.ds(h * hy, hy), k], got_az, at_z)
    b_chain = scatter_ring(NY, y, lambda k, h: pick_b.at[k, pl.ds(h * hz, hz)], got_by, at_y)
    advance(b_chain, 1)
    advance(a_chain, 1)
    advance(a_chain, 1)
    advance(b_chain, 1)
    advance(a_chain, 1)
    drain(b_chain)
    b_near = scatter_straight(NZ, z, lambda k: pick_b.at[y, k], got_bz, at_z, straight_sem.at[0])
    advance(b_near, 1)
    drain(a_chain)
    a_near = scatter_straight(NY, y, lambda k: pick_a.at[k, z], got_ay, at_y, straight_sem.at[1])
    advance(a_near, 1)
    drain(b_near)
    seen_b[y, z] = pick_b[y, z]
    b_near = gather_straight(NZ, z, lambda k: seen_b.at[y, k], at_z, straight_sem.at[2])
    advance(b_near, 1)
    drain(a_near)
    seen_a[y, z] = pick_a[y, z]
    a_near = gather_straight(NY, y, lambda k: seen_a.at[k, z], at_y, straight_sem.at[3])
    advance(a_near, 1)
    advance(w_chain, 1)
    drain(a_near)
    a_chain = gather_ring(NZ, z, lambda k, h: seen_a.at[pl.ds(h * hy, hy), k], at_z)
    advance(a_chain, 1)
    drain(b_near)
    b_chain = gather_ring(NY, y, lambda k, h: seen_b.at[k, pl.ds(h * hz, hz)], at_y)
    advance(b_chain, 1)
    advance(a_chain, 1)
    advance(a_chain, 1)
    advance(b_chain, 1)
    advance(a_chain, 1)
    drain(b_chain)
    drain(a_chain)

    seen_rows = obs_all
    high_ids = lax.broadcasted_iota(jnp.int32, (128, observations), 0)
    is_high = (high_ids == seen_rows // 128).astype(BF16)
    is_low = high_ids == seen_rows % 128
    seen_at = [jnp.sum(jnp.where(is_low, dot(table[i].astype(F32).T.astype(BF16), is_high), 0.0), axis=0, keepdims=True)
               for i in (0, 1)]
    row_start = pl.multiple_of(rows * block_rows + xl * 128, 128)
    near = coords[:, pl.ds(row_start, 128)].astype(F32)
    near = jnp.concatenate([near] * 4, axis=0).T
    own = near.shape[0] // 2
    row_at = jnp.where(core == 0, near[:own], near[own:])


    def covariance(k):
        o = [seen[k].reshape(per, seen.shape[3]) for seen in (seen_a, seen_b)]
        c = dot3([ref[...].reshape(2 * block_rows, half_members) for ref in (s_high, s_low)],
                 split(jnp.concatenate(o, axis=1)), NT)
        cross[k] = c.reshape(NX, 2, own, per).swapaxes(0, 1)
        pair = put(cross.at[k, 1 - core], cross_in.at[k], at_x(x, 1 - core))
        yield
        pair.wait_recv()
        cross[k, core] += cross_in[k]
        yield from scatter_ring(
            NX, x, lambda i, h: cross.at[k, core, i, pl.ds(h * (own // 2), own // 2)], got_x.at[k],
            lambda i: at_x(i, core))
        cols = slice(k * per, (k + 1) * per)
        apart_x = row_at[:, 0:1] - seen_at[0][:, cols]
        apart_y = row_at[:, 1:2] - seen_at[1][:, cols]
        reach = jnp.maximum(0.0, 1.0 - (apart_x * apart_x + apart_y * apart_y) / float(RADIUS * RADIUS))
        t_all[k, mem] = cross[k, core, x] * (reach * reach)
        across = put(t_all.at[k, mem], t_all.at[k, mem], at_x(xh * 2 + 1 - xl, core), t_all.at[k, (1 - xl) * 2 + core])
        beside = put(t_all.at[k, mem], t_all.at[k, mem], at_x(x, 1 - core), t_all.at[k, xl * 2 + 1 - core])
        yield
        across.wait_recv()
        there = (1 - xl) * 2
        passed = put(t_all.at[k, there + core], t_all.at[k, there + core], at_x(x, 1 - core),
                     t_all.at[k, there + 1 - core])
        yield
        beside.wait_recv()
        passed.wait_recv()

    for _ in turns([covariance(k) for k in range(NY)]):
        advance(w_chain, 1)
    drain(w_chain)

    t = [split(t_all[k].reshape(block_rows, per)) for k in range(NY)]
    t = [jnp.concatenate([piece[i] for piece in t], axis=1) for i in (0, 1)]
    step = 256
    for buf, start in ((w_a, 0), (w_b, width_a)):
        for k in range(buf.shape[3] // step):
            w = split(buf[:, :, :, k * step : (k + 1) * step].reshape(observations, step))
            out[:, start + k * step : start + (k + 1) * step] = dot3(t, w)

    for group in range(SENDS):
        all_lines(sum(sent[group::SENDS]), send_sem.at[group]).wait_send()
    assert count[0] == COPIES, count[0]
    assert max(sum(sent[group::SENDS]) for group in range(SENDS)) <= ledger.shape[0]


def on_device(state, member_level, level_weight, obs_row, state_coords, weights):
    block_rows, members = state.shape
    observations = obs_row.shape[0]
    half = members // 2
    own = block_rows // 4
    per = 2 * weights.shape[0]
    a, b = half * 3 // 5, half * 2 // 5
    hy, hz = NY // 2, NZ // 2
    line = observations // NY
    vmem = pl.BlockSpec(memory_space=pltpu.VMEM)
    smem = pl.BlockSpec(memory_space=pltpu.SMEM)
    hbm = pl.BlockSpec(memory_space=pltpu.HBM)
    return pl.pallas_call(
        kernel,
        out_shape=jax.ShapeDtypeStruct((block_rows, members), F32),
        in_specs=[hbm, hbm, smem, hbm, hbm, hbm],
        out_specs=vmem,
        scratch_shapes=[
            pltpu.VMEM(state.shape, F32),
            pltpu.VMEM(member_level.shape, jnp.int32),
            pltpu.VMEM(obs_row.shape, jnp.int32),
            pltpu.VMEM(state_coords.shape, jnp.int32),
            pltpu.VMEM(weights.shape, F32),
            pltpu.VMEM((2, state_coords.shape[1] // 128, 128), jnp.int32),
            pltpu.VMEM((NX * 2, 8, block_rows), F32),
            pltpu.VMEM((2, block_rows, half), F32),
            pltpu.VMEM((PIECES, block_rows // PIECES, half), F32),
            pltpu.VMEM((2, block_rows, half), BF16),
            pltpu.VMEM((2, block_rows, half), BF16),
            pltpu.VMEM((NY, NZ, per, a), F32),
            pltpu.VMEM((NY, NZ, per, b), F32),
            pltpu.VMEM((2, 2, hz, hy, per, a), F32),
            pltpu.VMEM((NY - 1, per, a), F32),
            pltpu.VMEM((2, 2, hy, hz, per, b), F32),
            pltpu.VMEM((NZ - 1, per, b), F32),
            pltpu.VMEM((NY, NZ, per, a), F32),
            pltpu.VMEM((NY, NZ, per, b), F32),
            pltpu.VMEM((NY, NZ, per, members * 2 // 5), F32),
            pltpu.VMEM((NY, NZ, per, members * 3 // 5), F32),
            pltpu.VMEM((NY, 2, NX, own, line), F32),
            pltpu.VMEM((NY, NX, own, line), F32),
            pltpu.VMEM((NY, 2, 2, 2, own // 2, line), F32),
            pltpu.VMEM((NY, 4, own, line), F32),
            pltpu.VMEM((2816, 128), F32),
            pltpu.SemaphoreType.DMA((SENDS,)),
            pltpu.SemaphoreType.DMA((COPIES,)),
            pltpu.SemaphoreType.DMA((STRAIGHT,)),
            pltpu.SemaphoreType.DMA((5,)),
        ],
        compiler_params=pltpu.CompilerParams(
            collective_id=0, has_side_effects=True, vmem_limit_bytes=VMEM_BYTES),
    )(
        state, member_level, level_weight, obs_row, state_coords, weights,
    )


def solution(mesh):
    return jax.shard_map(
        on_device,
        mesh=mesh,
        in_specs=(P("rows", "mem"), P("mem"), P(), P(), P(), P("rows", "mem")),
        out_specs=P("rows", "mem"),
        check_vma=False,
    )
```

```python
import math

import jax
import jax.numpy as jnp
from jax import lax
from jax.experimental import pallas as pl
from jax.experimental.pallas import tpu as pltpu
from jax.sharding import PartitionSpec as P

MESH = pl.DeviceIdType.MESH
LEVELS = 4
NX, NY, NZ = 4, 4, 8
RADIUS = 256
F32 = jnp.float32
BF16 = jnp.bfloat16
NT = (((1,), (1,)), ((), ()))
NN = (((1,), (0,)), ((), ()))
COPIES = 229
PIECES = 8
VMEM_BYTES = 67043328
SENDS = 16
STRAIGHT = 4


def split(value):
    high = value.astype(BF16)
    return high, (value - high.astype(F32)).astype(BF16)


def dot(a, b, dims=NN):
    return lax.dot_general(a, b, dims, preferred_element_type=F32)


def dot3(a, b, dims=NN):
    return dot(a[0], b[0], dims) + dot(a[0], b[1], dims) + dot(a[1], b[0], dims)


def turns(chains):
    chains = list(chains)
    while chains:
        left = []
        for chain in chains:
            try:
                next(chain)
                left.append(chain)
            except StopIteration:
                pass
        chains = left
        if chains:
            yield


def drain(chain):
    for _ in chain:
        pass


def advance(chain, count):
    for _ in range(count):
        next(chain, None)


def kernel(
    state_far, level_far, level_weight, obs_far, coords_far, w_far,
    out,
    state, level_line, obs_line, coords, w_in, table,
    sums, kept, relay, s_high, s_low, pick_a, pick_b, got_az, got_ay, got_by, got_bz,
    seen_a, seen_b, w_a, w_b, cross, cross_in, got_x, t_all, seen_at, total_out, ledger, send_sem, recv_sem, straight_sem, load_sem,
):
    rows, mem = lax.axis_index("rows"), lax.axis_index("mem")
    y, z, xh = rows // (NZ * 2), (rows // 2) % NZ, rows % 2
    xl, core = mem // 2, mem % 2
    x = xh * 2 + xl
    count = [0]
    sent, leaving = [], []

    def at_y(k):
        return ((k * NZ + z) * 2 + xh, mem)

    def at_z(k):
        return ((y * NZ + k) * 2 + xh, mem)

    def at_x(k, c):
        return ((y * NZ + z) * 2 + k // 2, (k % 2) * 2 + c)

    def put(src, dst, device, landing=None, arrival=None):
        recv = recv_sem.at[count[0]]
        if arrival is None:
            arrival = recv
            count[0] += 1
        group = len(sent) % SENDS
        copy = pltpu.make_async_remote_copy(
            src_ref=src, dst_ref=dst, send_sem=send_sem.at[group], recv_sem=arrival,
            device_id=device, device_id_type=MESH)
        copy.start()
        sent.append(math.prod(src.shape) // 128)
        if arrival is not recv:
            return None
        landing = dst if landing is None else landing
        return pltpu.make_async_remote_copy(
            src_ref=landing, dst_ref=landing, send_sem=send_sem.at[group],
            recv_sem=arrival, device_id=device, device_id_type=MESH)

    def all_lines(lines, semaphore):
        whole = ledger.at[pl.ds(0, lines)]
        return pltpu.make_async_remote_copy(
            src_ref=whole, dst_ref=whole, send_sem=semaphore, recv_sem=semaphore,
            device_id=at_x(x, 1 - core), device_id_type=MESH)

    def gather_ring(n, p, block, device, only=None, late=False):
        def chain(way, half):
            hops = n // 2 if (half == 0) == (way == 1) else n // 2 - 1
            arriving = None
            for s in range(1, hops + 1):
                if arriving is not None:
                    arriving.wait_recv()
                out_block = block((p - way * (s - 1) + n) % n, half)
                in_block = block((p - way * s + n) % n, half)
                arriving = put(out_block, out_block, device((p + way + n) % n), in_block)
                yield
            if late and hops < n // 2:
                yield
            if arriving is not None:
                arriving.wait_recv()
        order = [(1, 0), (-1, 1), (1, 1), (-1, 0)]
        return turns([chain(way, half) for way, half in order if only in (None, half)])

    def scatter_ring(n, p, block, landing, device):
        def chain(way, half):
            hops = n // 2 if (half == 0) == (way == 1) else n // 2 - 1
            direction = 0 if way == 1 else 1
            arriving = None
            for s in range(1, hops + 1):
                part = block((p + way * (hops - s + 1) + n) % n, half)
                if arriving is not None:
                    arriving.wait_recv()
                    part[...] += landing[direction, half, s - 2]
                arriving = put(part, landing.at[direction, half, s - 1], device((p + way + n) % n))
                yield
            if hops < n // 2:
                yield
            if arriving is not None:
                arriving.wait_recv()
                block(p, half)[...] += landing[direction, half, hops - 1]
        return turns([chain(1, 0), chain(-1, 1), chain(1, 1), chain(-1, 0)])

    def far_first(n):
        return sorted(range(1, n), key=lambda d: abs(d - n // 2))

    def scatter_straight(n, p, block, landing, device, arrival):
        for d in far_first(n):
            q = (p + d) % n
            put(block(q), landing.at[d - 1], device(q), arrival=arrival)
        yield
        all_lines((n - 1) * math.prod(landing.shape[1:]) // 128, arrival).wait_recv()
        block(p)[...] += sum(landing[d - 1] for d in range(1, n))

    def gather_straight(n, p, block, device, arrival):
        for d in far_first(n):
            put(block(p), block(p), device((p + d) % n), arrival=arrival)
        yield
        all_lines((n - 1) * math.prod(block(p).shape) // 128, arrival).wait_recv()

    def gather_fine(n, p, outer, inner):
        going, done, r = [inner(p)], False, 0
        while going or not done:
            if not done:
                try:
                    next(outer)
                except StopIteration:
                    done = True
                if r > 0:
                    going.append(inner((p + r) % n))
                    if 2 * r < n:
                        going.append(inner((p - r + n) % n))
                r += 1
            left = []
            for chain in going:
                try:
                    next(chain)
                    left.append(chain)
                except StopIteration:
                    pass
            going = left
            yield

    def part(h):
        return pl.ds((h + xh) % 2 * w_in.shape[0], w_in.shape[0])

    def y_outer(buf, own):
        return gather_fine(
            NY, y, gather_ring(NY, y, lambda k, h: buf.at[k, z, part(h)], at_y, own),
            lambda j: gather_ring(NZ, z, lambda k, h: buf.at[j, k, part(h)], at_z, own))

    def z_outer(buf, own):
        return gather_fine(
            NZ, z, gather_ring(NZ, z, lambda k, h: buf.at[y, k, part(h)], at_z, own),
            lambda j: gather_ring(NY, y, lambda k, h: buf.at[k, j, part(h)], at_y, own))

    friends = [at_y((y + 1) % NY), at_y((y + NY - 1) % NY), at_z((z + 1) % NZ), at_z((z + NZ - 1) % NZ)]
    line = [at_x((x + d) % NX, c) for d in range(1, NX) for c in (core, 1 - core)]
    line.append(at_x(x, 1 - core))
    barrier = pltpu.get_barrier_semaphore()
    for device in friends + line:
        pl.semaphore_signal(barrier, inc=1, device_id=device, device_id_type=MESH)

    loads = [pltpu.make_async_copy(far, near, load_sem.at[n]) for n, (far, near) in enumerate((
        (w_far, w_in), (state_far, state), (level_far, level_line), (obs_far, obs_line), (coords_far, coords)))]
    for load in loads:
        load.start()
    block_rows, members = state.shape
    half_members = members // 2
    observations = obs_line.shape[0]
    loads[0].wait()
    depth, width_a = w_in.shape[0], w_a.shape[3]
    w_a[y, z, pl.ds(xh * depth, depth)] = w_in[:, :width_a]
    w_b[y, z, pl.ds(xh * depth, depth)] = w_in[:, width_a:]
    mine = pl.ds(pl.multiple_of(xh * half_members, 128), half_members)
    theirs = pl.ds(pl.multiple_of((1 - xh) * half_members, 128), half_members)

    for load in loads[1:]:
        load.wait()
    level_all = level_line[...].reshape(1, members)
    obs_all = obs_line[...].reshape(1, observations)
    pl.semaphore_wait(barrier, len(friends) + len(line))

    partner = at_x((x + 2) % NX, core)
    own_part, other_part = pl.ds(xh * depth, depth), pl.ds((1 - xh) * depth, depth)
    w_pair = [put(buf.at[y, z, own_part], buf.at[y, z, own_part], partner, buf.at[y, z, other_part]) for buf in (w_b, w_a)]
    piece = block_rows // PIECES
    hops = []
    for n in range(PIECES):
        k = n // 2 + (n % 2) * (PIECES // 2)
        way = 1 if n % 2 == 0 else NX - 1
        hops.append((k, way, put(state.at[pl.ds(k * piece, piece), theirs], relay.at[k], at_x((x + way) % NX, core))))

    def pass_on(numbers):
        landed = []
        for n in numbers:
            k, way, arriving = hops[n]
            arriving.wait_recv()
            origin = ((x - way + NX) % NX) // 2
            spot = pl.ds(k * piece, piece)
            landed.append(put(relay.at[k], kept.at[origin, spot], at_x((x + way) % NX, core), kept.at[1 - xh, spot]))
        return landed

    w_own = turns([z_outer(w_b, 0), y_outer(w_a, 0)])
    w_other = turns([z_outer(w_b, 1), y_outer(w_a, 1)])
    advance(w_own, 1)
    level_ids = lax.broadcasted_iota(jnp.int32, (8, members), 0)
    own_level = level_all
    onehot = (level_ids == own_level).astype(F32)
    counted = jnp.sum((level_ids - LEVELS == own_level).astype(F32), axis=1, keepdims=True)
    summed = lax.dot_general(onehot, state[...], NT, precision=lax.Precision.HIGHEST, preferred_element_type=F32)
    sums[x * 2 + core] = summed + counted
    sums_in = []
    for d in range(1, NX):
        for c in (0, 1):
            device = at_x((x + d) % NX, (core + c) % 2)
            from_x, from_core = (x - d + NX) % NX, (core + c) % 2
            sums_in.append(put(sums.at[x * 2 + core], sums.at[x * 2 + core], device, sums.at[from_x * 2 + from_core]))
    sums_in.append(put(sums.at[x * 2 + core], sums.at[x * 2 + core], at_x(x, 1 - core), sums.at[x * 2 + 1 - core]))
    kept[xh] = state[:, mine]
    kept_level = jnp.where(xh == 0, level_all[:, :half_members], level_all[:, half_members:])
    block = rows // 2
    obs_col = jnp.broadcast_to(obs_all, (8, observations)).T[:, 0:1]

    advance(w_own, 1)
    for arriving in w_pair:
        arriving.wait_recv()
    advance(w_other, 1)
    landed = pass_on(range(0, PIECES // 2))
    advance(w_other, 1)
    landed += pass_on(range(PIECES // 2, PIECES))
    advance(w_own, 1)
    for k in range(table.shape[1]):
        table[:, k, :] = coords[:, k * 128 : (k + 1) * 128]
    for arriving in sums_in:
        arriving.wait_recv()
    total = [sums[h * 4] + sums[h * 4 + 1] + sums[h * 4 + 2] + sums[h * 4 + 3] for h in (0, 1)]
    means = [(t / jnp.concatenate([t[LEVELS:], t[LEVELS:]], axis=0)).T for t in total]
    scale = jnp.zeros((1, half_members), F32)
    for l in range(LEVELS):
        value = level_weight[l] / (total[0][LEVELS + l : LEVELS + l + 1, 0:1] - 1.0)
        scale = jnp.where(kept_level == l, value, scale)

    wide_a = pick_a.shape[3]
    per = NZ * pick_a.shape[2]

    def prepare(h, first):
        mean = jnp.where(h == 0, means[0], means[1])
        shift = jnp.zeros((block_rows, half_members), F32)
        for l in range(LEVELS):
            shift = jnp.where(kept_level == l, mean[:, l : l + 1], shift)
        anomaly = kept[h] - shift
        s_high[h], s_low[h] = split(anomaly * scale)
        high, low = split(anomaly)
        row_ids = lax.broadcasted_iota(jnp.int32, (per, block_rows), 1) + (block * 2 + h) * block_rows
        for k in range(NY):
            chosen = (obs_col[k * per : (k + 1) * per] == row_ids).astype(BF16)
            picked = dot(chosen, high) + dot(chosen, low)
            a = picked[:, :wide_a].reshape(NZ, per // NZ, wide_a)
            b = picked[:, wide_a:].reshape(NZ, per // NZ, half_members - wide_a)
            pick_a[k] = a if first else pick_a[k] + a
            pick_b[k] = b if first else pick_b[k] + b

    prepare(xh, True)
    advance(w_other, 1)
    w_chain = turns([w_own, w_other])
    for arriving in landed:
        arriving.wait_recv()
    prepare(1 - xh, False)

    nb = pick_a.shape[2] // 2
    hy, hz = NY // 2, NZ // 2
    a_chain = scatter_ring(NZ, z, lambda k, h: pick_a.at[pl.ds(h * hy, hy), k], got_az, at_z)
    b_chain = scatter_ring(NY, y, lambda k, h: pick_b.at[k, pl.ds(h * hz, hz)], got_by, at_y)
    advance(b_chain, 1)
    advance(a_chain, 1)
    advance(a_chain, 1)
    advance(b_chain, 1)
    advance(a_chain, 1)
    advance(a_chain, 1)
    drain(b_chain)
    b_near = scatter_straight(NZ, z, lambda k: pick_b.at[y, k], got_bz, at_z, straight_sem.at[0])
    advance(b_near, 1)
    drain(a_chain)
    a_near = scatter_straight(NY, y, lambda k: pick_a.at[k, z], got_ay, at_y, straight_sem.at[1])
    advance(a_near, 1)
    seen_rows = obs_all
    high_ids = lax.broadcasted_iota(jnp.int32, (128, observations), 0)
    is_high = (high_ids == seen_rows // 128).astype(BF16)
    is_low = high_ids == seen_rows % 128
    for i in (0, 1):
        found = dot(table[i].astype(F32).T.astype(BF16), is_high)
        found = jnp.sum(jnp.where(is_low, found, 0.0), axis=0, keepdims=True)
        for k in range(NY):
            seen_at[i, k] = found[:, k * per : (k + 1) * per]
    row_start = pl.multiple_of(rows * block_rows + xl * 128, 128)
    near = coords[:, pl.ds(row_start, 128)].astype(F32)
    near = jnp.concatenate([near] * 4, axis=0).T
    own = near.shape[0] // 2
    row_at = jnp.where(core == 0, near[:own], near[own:])


    drain(a_near)
    seen_a[y, z] = pick_a[y, z]
    a_near = gather_straight(NY, y, lambda k: seen_a.at[k, z], at_y, straight_sem.at[3])
    advance(a_near, 1)
    drain(b_near)
    seen_b[y, z] = pick_b[y, z]
    b_near = gather_straight(NZ, z, lambda k: seen_b.at[y, k], at_z, straight_sem.at[2])
    advance(b_near, 1)
    drain(a_near)
    a_chain = gather_ring(NZ, z, lambda k, h: seen_a.at[pl.ds(h * hy, hy), k], at_z, late=True)
    advance(a_chain, 1)
    drain(b_near)
    b_chain = gather_ring(NY, y, lambda k, h: seen_b.at[k, pl.ds(h * hz, hz)], at_y)
    advance(b_chain, 1)
    advance(a_chain, 1)
    advance(a_chain, 1)
    advance(a_chain, 1)
    advance(b_chain, 1)
    drain(a_chain)

    def covariance(k):
        there_y = (y + k) % NY
        o = [seen[there_y].reshape(per, seen.shape[3]) for seen in (seen_a, seen_b)]
        c = dot3([ref[...].reshape(2 * block_rows, half_members) for ref in (s_high, s_low)],
                 split(jnp.concatenate(o, axis=1)), NT)
        cross[k] = c.reshape(NX, 2, own, per).swapaxes(0, 1)
        pair = put(cross.at[k, 1 - core], cross_in.at[k], at_x(x, 1 - core))
        yield
        pair.wait_recv()
        cross[k, core] += cross_in[k]
        yield from scatter_ring(
            NX, x, lambda i, h: cross.at[k, core, i, pl.ds(h * (own // 2), own // 2)], got_x.at[k],
            lambda i: at_x(i, core))
        apart_x = row_at[:, 0:1] - seen_at[0, there_y]
        apart_y = row_at[:, 1:2] - seen_at[1, there_y]
        reach = jnp.maximum(0.0, 1.0 - (apart_x * apart_x + apart_y * apart_y) / float(RADIUS * RADIUS))
        t_all[k, mem] = cross[k, core, x] * (reach * reach)
        across = put(t_all.at[k, mem], t_all.at[k, mem], at_x(xh * 2 + 1 - xl, core), t_all.at[k, (1 - xl) * 2 + core])
        beside = put(t_all.at[k, mem], t_all.at[k, mem], at_x(x, 1 - core), t_all.at[k, xl * 2 + 1 - core])
        yield
        across.wait_recv()
        there = (1 - xl) * 2
        passed = put(t_all.at[k, there + core], t_all.at[k, there + core], at_x(x, 1 - core),
                     t_all.at[k, there + 1 - core])
        yield
        beside.wait_recv()
        passed.wait_recv()
        drain(w_chain)
        t = split(t_all[k].reshape(block_rows, per))
        step = 256
        for buf, start in ((w_a, 0), (w_b, width_a)):
            for n in range(buf.shape[3] // step):
                w = split(buf[there_y, :, :, n * step : (n + 1) * step].reshape(per, step))
                cols = slice(start + n * step, start + (n + 1) * step)
                if k == 0:
                    total_out[:, cols] = dot3(t, w)
                else:
                    total_out[:, cols] += dot3(t, w)
                if k == NY // 2:
                    leaving.append(pltpu.make_async_copy(
                        total_out.at[:, pl.ds(cols.start, step)], out.at[:, pl.ds(cols.start, step)],
                        load_sem.at[len(leaving)]))
                    leaving[-1].start()

    chains = [covariance(k) for k in range(NY)]
    near_first = [0, 1, 3, 2]
    next(chains[0])
    advance(w_chain, 1)
    next(chains[1])
    next(chains[3])
    for k in near_first[:3]:
        next(chains[k])
    drain(b_chain)
    next(chains[2])
    advance(w_chain, 1)
    for n, _ in enumerate(turns([chains[k] for k in near_first])):
        advance(w_chain, 1)
    for copy in leaving:
        copy.wait()
    for group in range(SENDS):
        all_lines(sum(sent[group::SENDS]), send_sem.at[group]).wait_send()
    assert count[0] == COPIES, count[0]
    assert max(sum(sent[group::SENDS]) for group in range(SENDS)) <= ledger.shape[0]


def on_device(state, member_level, level_weight, obs_row, state_coords, weights):
    block_rows, members = state.shape
    observations = obs_row.shape[0]
    half = members // 2
    own = block_rows // 4
    per = 2 * weights.shape[0]
    a, b = half * 2 // 5, half * 3 // 5
    hy, hz = NY // 2, NZ // 2
    line = observations // NY
    smem = pl.BlockSpec(memory_space=pltpu.SMEM)
    hbm = pl.BlockSpec(memory_space=pltpu.HBM)
    return pl.pallas_call(
        kernel,
        out_shape=jax.ShapeDtypeStruct((block_rows, members), F32),
        in_specs=[hbm, hbm, smem, hbm, hbm, hbm],
        out_specs=hbm,
        scratch_shapes=[
            pltpu.VMEM(state.shape, F32),
            pltpu.VMEM(member_level.shape, jnp.int32),
            pltpu.VMEM(obs_row.shape, jnp.int32),
            pltpu.VMEM(state_coords.shape, jnp.int32),
            pltpu.VMEM(weights.shape, F32),
            pltpu.VMEM((2, state_coords.shape[1] // 128, 128), jnp.int32),
            pltpu.VMEM((NX * 2, 8, block_rows), F32),
            pltpu.VMEM((2, block_rows, half), F32),
            pltpu.VMEM((PIECES, block_rows // PIECES, half), F32),
            pltpu.VMEM((2, block_rows, half), BF16),
            pltpu.VMEM((2, block_rows, half), BF16),
            pltpu.VMEM((NY, NZ, per, a), F32),
            pltpu.VMEM((NY, NZ, per, b), F32),
            pltpu.VMEM((2, 2, hz, hy, per, a), F32),
            pltpu.VMEM((NY - 1, per, a), F32),
            pltpu.VMEM((2, 2, hy, hz, per, b), F32),
            pltpu.VMEM((NZ - 1, per, b), F32),
            pltpu.VMEM((NY, NZ, per, a), F32),
            pltpu.VMEM((NY, NZ, per, b), F32),
            pltpu.VMEM((NY, NZ, per, members * 2 // 5), F32),
            pltpu.VMEM((NY, NZ, per, members * 3 // 5), F32),
            pltpu.VMEM((NY, 2, NX, own, line), F32),
            pltpu.VMEM((NY, NX, own, line), F32),
            pltpu.VMEM((NY, 2, 2, 2, own // 2, line), F32),
            pltpu.VMEM((NY, 4, own, line), F32),
            pltpu.VMEM((2, NY, 1, line), F32),
            pltpu.VMEM(state.shape, F32),
            pltpu.VMEM((2816, 128), F32),
            pltpu.SemaphoreType.DMA((SENDS,)),
            pltpu.SemaphoreType.DMA((COPIES,)),
            pltpu.SemaphoreType.DMA((STRAIGHT,)),
            pltpu.SemaphoreType.DMA((5,)),
        ],
        compiler_params=pltpu.CompilerParams(
            collective_id=0, has_side_effects=True, vmem_limit_bytes=VMEM_BYTES),
    )(
        state, member_level, level_weight, obs_row, state_coords, weights,
    )


def solution(mesh):
    return jax.shard_map(
        on_device,
        mesh=mesh,
        in_specs=(P("rows", "mem"), P("mem"), P(), P(), P(), P("rows", "mem")),
        out_specs=P("rows", "mem"),
        check_vma=False,
    )
```

```python
import math

import jax
import jax.numpy as jnp
from jax import lax
from jax.experimental import pallas as pl
from jax.experimental.pallas import tpu as pltpu
from jax.sharding import PartitionSpec as P

MESH = pl.DeviceIdType.MESH
LEVELS = 4
NX, NY, NZ = 4, 4, 8
RADIUS = 256
F32 = jnp.float32
BF16 = jnp.bfloat16
NT = (((1,), (1,)), ((), ()))
NN = (((1,), (0,)), ((), ()))
COPIES = 229
PIECES = 8
VMEM_BYTES = 67043328
SENDS = 16
STRAIGHT = 4


def split(value):
    high = value.astype(BF16)
    return high, (value - high.astype(F32)).astype(BF16)


def dot(a, b, dims=NN):
    return lax.dot_general(a, b, dims, preferred_element_type=F32)


def dot3(a, b, dims=NN):
    return dot(a[0], b[0], dims) + dot(a[0], b[1], dims) + dot(a[1], b[0], dims)


def turns(chains):
    chains = list(chains)
    while chains:
        left = []
        for chain in chains:
            try:
                next(chain)
                left.append(chain)
            except StopIteration:
                pass
        chains = left
        if chains:
            yield


def drain(chain):
    for _ in chain:
        pass


def advance(chain, count):
    for _ in range(count):
        next(chain, None)


def kernel(
    state_far, level_far, level_weight, obs_far, coords_far, w_far,
    out,
    state, level_line, obs_line, coords, w_in, table,
    sums, kept, relay, s_high, s_low, pick_a, pick_b, got_az, got_ay, got_by, got_bz,
    seen_a, seen_b, w_a, w_b, cross, cross_in, got_x, t_all, seen_at, total_out, ledger, send_sem, recv_sem, straight_sem, load_sem,
):
    rows, mem = lax.axis_index("rows"), lax.axis_index("mem")
    y, z, xh = rows // (NZ * 2), (rows // 2) % NZ, rows % 2
    xl, core = mem // 2, mem % 2
    x = xh * 2 + xl
    count = [0]
    sent, leaving = [], []

    def at_y(k):
        return ((k * NZ + z) * 2 + xh, mem)

    def at_z(k):
        return ((y * NZ + k) * 2 + xh, mem)

    def at_x(k, c):
        return ((y * NZ + z) * 2 + k // 2, (k % 2) * 2 + c)

    def put(src, dst, device, landing=None, arrival=None):
        recv = recv_sem.at[count[0]]
        if arrival is None:
            arrival = recv
            count[0] += 1
        group = len(sent) % SENDS
        copy = pltpu.make_async_remote_copy(
            src_ref=src, dst_ref=dst, send_sem=send_sem.at[group], recv_sem=arrival,
            device_id=device, device_id_type=MESH)
        copy.start()
        sent.append(math.prod(src.shape) // 128)
        if arrival is not recv:
            return None
        landing = dst if landing is None else landing
        return pltpu.make_async_remote_copy(
            src_ref=landing, dst_ref=landing, send_sem=send_sem.at[group],
            recv_sem=arrival, device_id=device, device_id_type=MESH)

    def all_lines(lines, semaphore):
        whole = ledger.at[pl.ds(0, lines)]
        return pltpu.make_async_remote_copy(
            src_ref=whole, dst_ref=whole, send_sem=semaphore, recv_sem=semaphore,
            device_id=at_x(x, 1 - core), device_id_type=MESH)

    def gather_ring(n, p, block, device, only=None, late=False):
        def chain(way, half):
            hops = n // 2 if (half == 0) == (way == 1) else n // 2 - 1
            arriving = None
            for s in range(1, hops + 1):
                if arriving is not None:
                    arriving.wait_recv()
                out_block = block((p - way * (s - 1) + n) % n, half)
                in_block = block((p - way * s + n) % n, half)
                arriving = put(out_block, out_block, device((p + way + n) % n), in_block)
                yield
            if late and hops < n // 2:
                yield
            if arriving is not None:
                arriving.wait_recv()
        order = [(1, 0), (-1, 1), (1, 1), (-1, 0)]
        return turns([chain(way, half) for way, half in order if only in (None, half)])

    def scatter_ring(n, p, block, landing, device):
        def chain(way, half):
            hops = n // 2 if (half == 0) == (way == 1) else n // 2 - 1
            direction = 0 if way == 1 else 1
            arriving = None
            for s in range(1, hops + 1):
                part = block((p + way * (hops - s + 1) + n) % n, half)
                if arriving is not None:
                    arriving.wait_recv()
                    part[...] += landing[direction, half, s - 2]
                arriving = put(part, landing.at[direction, half, s - 1], device((p + way + n) % n))
                yield
            if hops < n // 2:
                yield
            if arriving is not None:
                arriving.wait_recv()
                block(p, half)[...] += landing[direction, half, hops - 1]
        return turns([chain(1, 0), chain(-1, 1), chain(1, 1), chain(-1, 0)])

    def far_first(n):
        return sorted(range(1, n), key=lambda d: abs(d - n // 2))

    def scatter_straight(n, p, block, landing, device, arrival):
        for d in far_first(n):
            q = (p + d) % n
            put(block(q), landing.at[d - 1], device(q), arrival=arrival)
        yield
        all_lines((n - 1) * math.prod(landing.shape[1:]) // 128, arrival).wait_recv()
        block(p)[...] += sum(landing[d - 1] for d in range(1, n))

    def gather_straight(n, p, block, device, arrival):
        for d in far_first(n):
            put(block(p), block(p), device((p + d) % n), arrival=arrival)
        yield
        all_lines((n - 1) * math.prod(block(p).shape) // 128, arrival).wait_recv()

    def gather_fine(n, p, outer, inner):
        going, done, r = [inner(p)], False, 0
        while going or not done:
            if not done:
                try:
                    next(outer)
                except StopIteration:
                    done = True
                if r > 0:
                    going.append(inner((p + r) % n))
                    if 2 * r < n:
                        going.append(inner((p - r + n) % n))
                r += 1
            left = []
            for chain in going:
                try:
                    next(chain)
                    left.append(chain)
                except StopIteration:
                    pass
            going = left
            yield

    def part(h):
        return pl.ds((h + xh) % 2 * w_in.shape[0], w_in.shape[0])

    def y_outer(buf, own):
        return gather_fine(
            NY, y, gather_ring(NY, y, lambda k, h: buf.at[k, z, part(h)], at_y, own),
            lambda j: gather_ring(NZ, z, lambda k, h: buf.at[j, k, part(h)], at_z, own))

    def z_outer(buf, own):
        return gather_fine(
            NZ, z, gather_ring(NZ, z, lambda k, h: buf.at[y, k, part(h)], at_z, own),
            lambda j: gather_ring(NY, y, lambda k, h: buf.at[k, j, part(h)], at_y, own))

    friends = [at_y((y + 1) % NY), at_y((y + NY - 1) % NY), at_z((z + 1) % NZ), at_z((z + NZ - 1) % NZ)]
    line = [at_x((x + d) % NX, c) for d in range(1, NX) for c in (core, 1 - core)]
    line.append(at_x(x, 1 - core))
    barrier = pltpu.get_barrier_semaphore()
    for device in friends + line:
        pl.semaphore_signal(barrier, inc=1, device_id=device, device_id_type=MESH)

    loads = [pltpu.make_async_copy(far, near, load_sem.at[n]) for n, (far, near) in enumerate((
        (w_far, w_in), (state_far, state), (level_far, level_line), (obs_far, obs_line), (coords_far, coords)))]
    for load in loads:
        load.start()
    block_rows, members = state.shape
    half_members = members // 2
    observations = obs_line.shape[0]
    loads[0].wait()
    depth, width_a = w_in.shape[0], w_a.shape[3]
    w_a[y, z, pl.ds(xh * depth, depth)] = w_in[:, :width_a]
    w_b[y, z, pl.ds(xh * depth, depth)] = w_in[:, width_a:]
    mine = pl.ds(pl.multiple_of(xh * half_members, 128), half_members)
    theirs = pl.ds(pl.multiple_of((1 - xh) * half_members, 128), half_members)

    for load in loads[1:]:
        load.wait()
    level_all = level_line[...].reshape(1, members)
    obs_all = obs_line[...].reshape(1, observations)
    pl.semaphore_wait(barrier, len(friends) + len(line))

    partner = at_x((x + 2) % NX, core)
    own_part, other_part = pl.ds(xh * depth, depth), pl.ds((1 - xh) * depth, depth)
    w_pair = [put(buf.at[y, z, own_part], buf.at[y, z, own_part], partner, buf.at[y, z, other_part]) for buf in (w_b, w_a)]
    piece = block_rows // PIECES
    hops = []
    for n in range(PIECES):
        k = n // 2 + (n % 2) * (PIECES // 2)
        way = 1 if n % 2 == 0 else NX - 1
        hops.append((k, way, put(state.at[pl.ds(k * piece, piece), theirs], relay.at[k], at_x((x + way) % NX, core))))

    def pass_on(numbers):
        landed = []
        for n in numbers:
            k, way, arriving = hops[n]
            arriving.wait_recv()
            origin = ((x - way + NX) % NX) // 2
            spot = pl.ds(k * piece, piece)
            landed.append(put(relay.at[k], kept.at[origin, spot], at_x((x + way) % NX, core), kept.at[1 - xh, spot]))
        return landed

    w_own = turns([z_outer(w_b, 0), y_outer(w_a, 0)])
    w_other = turns([z_outer(w_b, 1), y_outer(w_a, 1)])
    advance(w_own, 1)
    level_ids = lax.broadcasted_iota(jnp.int32, (8, members), 0)
    own_level = level_all
    onehot = (level_ids == own_level).astype(F32)
    counted = jnp.sum((level_ids - LEVELS == own_level).astype(F32), axis=1, keepdims=True)
    summed = lax.dot_general(onehot, state[...], NT, precision=lax.Precision.HIGHEST, preferred_element_type=F32)
    sums[x * 2 + core] = summed + counted
    sums_in = []
    for d in range(1, NX):
        for c in (0, 1):
            device = at_x((x + d) % NX, (core + c) % 2)
            from_x, from_core = (x - d + NX) % NX, (core + c) % 2
            sums_in.append(put(sums.at[x * 2 + core], sums.at[x * 2 + core], device, sums.at[from_x * 2 + from_core]))
    sums_in.append(put(sums.at[x * 2 + core], sums.at[x * 2 + core], at_x(x, 1 - core), sums.at[x * 2 + 1 - core]))
    kept[xh] = state[:, mine]
    kept_level = jnp.where(xh == 0, level_all[:, :half_members], level_all[:, half_members:])
    block = rows // 2
    obs_col = jnp.broadcast_to(obs_all, (8, observations)).T[:, 0:1]

    advance(w_own, 1)
    for arriving in w_pair:
        arriving.wait_recv()
    advance(w_other, 1)
    landed = pass_on(range(0, PIECES // 2))
    advance(w_other, 1)
    landed += pass_on(range(PIECES // 2, PIECES))
    advance(w_own, 1)
    for k in range(table.shape[1]):
        table[:, k, :] = coords[:, k * 128 : (k + 1) * 128]
    for arriving in sums_in:
        arriving.wait_recv()
    total = [sums[h * 4] + sums[h * 4 + 1] + sums[h * 4 + 2] + sums[h * 4 + 3] for h in (0, 1)]
    means = [(t / jnp.concatenate([t[LEVELS:], t[LEVELS:]], axis=0)).T for t in total]
    scale = jnp.zeros((1, half_members), F32)
    for l in range(LEVELS):
        value = level_weight[l] / (total[0][LEVELS + l : LEVELS + l + 1, 0:1] - 1.0)
        scale = jnp.where(kept_level == l, value, scale)

    wide_a = pick_a.shape[3]
    per = NZ * pick_a.shape[2]

    def prepare(h, first):
        mean = jnp.where(h == 0, means[0], means[1])
        shift = jnp.zeros((block_rows, half_members), F32)
        for l in range(LEVELS):
            shift = jnp.where(kept_level == l, mean[:, l : l + 1], shift)
        anomaly = kept[h] - shift
        s_high[h], s_low[h] = split(anomaly * scale)
        high, low = split(anomaly)
        row_ids = lax.broadcasted_iota(jnp.int32, (per, block_rows), 1) + (block * 2 + h) * block_rows
        for k in range(NY):
            chosen = (obs_col[k * per : (k + 1) * per] == row_ids).astype(BF16)
            picked = dot(chosen, high) + dot(chosen, low)
            a = picked[:, :wide_a].reshape(NZ, per // NZ, wide_a)
            b = picked[:, wide_a:].reshape(NZ, per // NZ, half_members - wide_a)
            pick_a[k] = a if first else pick_a[k] + a
            pick_b[k] = b if first else pick_b[k] + b

    prepare(xh, True)
    advance(w_other, 1)
    w_chain = turns([w_own, w_other])
    for arriving in landed:
        arriving.wait_recv()
    prepare(1 - xh, False)

    nb = pick_a.shape[2] // 2
    hy, hz = NY // 2, NZ // 2
    a_chain = scatter_ring(NZ, z, lambda k, h: pick_a.at[pl.ds(h * hy, hy), k], got_az, at_z)
    b_chain = scatter_ring(NY, y, lambda k, h: pick_b.at[k, pl.ds(h * hz, hz)], got_by, at_y)
    advance(b_chain, 1)
    advance(a_chain, 1)
    advance(a_chain, 1)
    advance(b_chain, 1)
    advance(a_chain, 1)
    advance(a_chain, 1)
    drain(b_chain)
    b_near = scatter_straight(NZ, z, lambda k: pick_b.at[y, k], got_bz, at_z, straight_sem.at[0])
    advance(b_near, 1)
    drain(a_chain)
    a_near = scatter_straight(NY, y, lambda k: pick_a.at[k, z], got_ay, at_y, straight_sem.at[1])
    advance(a_near, 1)
    seen_rows = obs_all
    high_ids = lax.broadcasted_iota(jnp.int32, (128, observations), 0)
    is_high = (high_ids == seen_rows // 128).astype(BF16)
    is_low = high_ids == seen_rows % 128
    for i in (0, 1):
        found = dot(table[i].astype(F32).T.astype(BF16), is_high)
        found = jnp.sum(jnp.where(is_low, found, 0.0), axis=0, keepdims=True)
        for k in range(NY):
            seen_at[i, k] = found[:, k * per : (k + 1) * per]
    row_start = pl.multiple_of(rows * block_rows + xl * 128, 128)
    near = coords[:, pl.ds(row_start, 128)].astype(F32)
    near = jnp.concatenate([near] * 4, axis=0).T
    own = near.shape[0] // 2
    row_at = jnp.where(core == 0, near[:own], near[own:])


    drain(a_near)
    seen_a[y, z] = pick_a[y, z]
    a_near = gather_straight(NY, y, lambda k: seen_a.at[k, z], at_y, straight_sem.at[3])
    advance(a_near, 1)
    drain(b_near)
    seen_b[y, z] = pick_b[y, z]
    b_near = gather_straight(NZ, z, lambda k: seen_b.at[y, k], at_z, straight_sem.at[2])
    advance(b_near, 1)
    drain(a_near)
    a_chain = gather_ring(NZ, z, lambda k, h: seen_a.at[pl.ds(h * hy, hy), k], at_z, late=True)
    advance(a_chain, 1)
    drain(b_near)
    b_chain = gather_ring(NY, y, lambda k, h: seen_b.at[k, pl.ds(h * hz, hz)], at_y)
    advance(b_chain, 1)
    advance(a_chain, 1)
    def partial(k, seen, cols, add):
        c = dot3([ref[:, :, cols].reshape(2 * block_rows, -1) for ref in (s_high, s_low)],
                 split(seen[(y + k) % NY].reshape(per, seen.shape[3])), NT)
        c = c.reshape(NX, 2, own, per).swapaxes(0, 1)
        cross[k] = cross[k] + c if add else c

    partial(0, seen_b, slice(wide_a, None), False)
    advance(a_chain, 1)
    advance(a_chain, 1)
    advance(b_chain, 1)
    partial(1, seen_b, slice(wide_a, None), False)
    partial(3, seen_b, slice(wide_a, None), False)
    drain(a_chain)

    def covariance(k):
        there_y = (y + k) % NY
        if k == NY // 2:
            partial(k, seen_b, slice(wide_a, None), False)
        partial(k, seen_a, slice(0, wide_a), True)
        pair = put(cross.at[k, 1 - core], cross_in.at[k], at_x(x, 1 - core))
        yield
        pair.wait_recv()
        cross[k, core] += cross_in[k]
        yield from scatter_ring(
            NX, x, lambda i, h: cross.at[k, core, i, pl.ds(h * (own // 2), own // 2)], got_x.at[k],
            lambda i: at_x(i, core))
        apart_x = row_at[:, 0:1] - seen_at[0, there_y]
        apart_y = row_at[:, 1:2] - seen_at[1, there_y]
        reach = jnp.maximum(0.0, 1.0 - (apart_x * apart_x + apart_y * apart_y) / float(RADIUS * RADIUS))
        t_all[k, mem] = cross[k, core, x] * (reach * reach)
        across = put(t_all.at[k, mem], t_all.at[k, mem], at_x(xh * 2 + 1 - xl, core), t_all.at[k, (1 - xl) * 2 + core])
        beside = put(t_all.at[k, mem], t_all.at[k, mem], at_x(x, 1 - core), t_all.at[k, xl * 2 + 1 - core])
        yield
        across.wait_recv()
        there = (1 - xl) * 2
        passed = put(t_all.at[k, there + core], t_all.at[k, there + core], at_x(x, 1 - core),
                     t_all.at[k, there + 1 - core])
        yield
        beside.wait_recv()
        passed.wait_recv()
        drain(w_chain)
        t = split(t_all[k].reshape(block_rows, per))
        step = 256
        for buf, start in ((w_a, 0), (w_b, width_a)):
            for n in range(buf.shape[3] // step):
                w = split(buf[there_y, :, :, n * step : (n + 1) * step].reshape(per, step))
                cols = slice(start + n * step, start + (n + 1) * step)
                if k == 0:
                    total_out[:, cols] = dot3(t, w)
                else:
                    total_out[:, cols] += dot3(t, w)
                if k == NY // 2:
                    leaving.append(pltpu.make_async_copy(
                        total_out.at[:, pl.ds(cols.start, step)], out.at[:, pl.ds(cols.start, step)],
                        load_sem.at[len(leaving)]))
                    leaving[-1].start()

    chains = [covariance(k) for k in range(NY)]
    near_first = [0, 1, 3, 2]
    next(chains[0])
    advance(w_chain, 1)
    next(chains[1])
    next(chains[3])
    for k in near_first[:3]:
        next(chains[k])
    drain(b_chain)
    next(chains[2])
    advance(w_chain, 1)
    for n, _ in enumerate(turns([chains[k] for k in near_first])):
        advance(w_chain, 1)
    for copy in leaving:
        copy.wait()
    for group in range(SENDS):
        all_lines(sum(sent[group::SENDS]), send_sem.at[group]).wait_send()
    assert count[0] == COPIES, count[0]
    assert max(sum(sent[group::SENDS]) for group in range(SENDS)) <= ledger.shape[0]


def on_device(state, member_level, level_weight, obs_row, state_coords, weights):
    block_rows, members = state.shape
    observations = obs_row.shape[0]
    half = members // 2
    own = block_rows // 4
    per = 2 * weights.shape[0]
    a, b = half * 2 // 5, half * 3 // 5
    hy, hz = NY // 2, NZ // 2
    line = observations // NY
    smem = pl.BlockSpec(memory_space=pltpu.SMEM)
    hbm = pl.BlockSpec(memory_space=pltpu.HBM)
    return pl.pallas_call(
        kernel,
        out_shape=jax.ShapeDtypeStruct((block_rows, members), F32),
        in_specs=[hbm, hbm, smem, hbm, hbm, hbm],
        out_specs=hbm,
        scratch_shapes=[
            pltpu.VMEM(state.shape, F32),
            pltpu.VMEM(member_level.shape, jnp.int32),
            pltpu.VMEM(obs_row.shape, jnp.int32),
            pltpu.VMEM(state_coords.shape, jnp.int32),
            pltpu.VMEM(weights.shape, F32),
            pltpu.VMEM((2, state_coords.shape[1] // 128, 128), jnp.int32),
            pltpu.VMEM((NX * 2, 8, block_rows), F32),
            pltpu.VMEM((2, block_rows, half), F32),
            pltpu.VMEM((PIECES, block_rows // PIECES, half), F32),
            pltpu.VMEM((2, block_rows, half), BF16),
            pltpu.VMEM((2, block_rows, half), BF16),
            pltpu.VMEM((NY, NZ, per, a), F32),
            pltpu.VMEM((NY, NZ, per, b), F32),
            pltpu.VMEM((2, 2, hz, hy, per, a), F32),
            pltpu.VMEM((NY - 1, per, a), F32),
            pltpu.VMEM((2, 2, hy, hz, per, b), F32),
            pltpu.VMEM((NZ - 1, per, b), F32),
            pltpu.VMEM((NY, NZ, per, a), F32),
            pltpu.VMEM((NY, NZ, per, b), F32),
            pltpu.VMEM((NY, NZ, per, members * 2 // 5), F32),
            pltpu.VMEM((NY, NZ, per, members * 3 // 5), F32),
            pltpu.VMEM((NY, 2, NX, own, line), F32),
            pltpu.VMEM((NY, NX, own, line), F32),
            pltpu.VMEM((NY, 2, 2, 2, own // 2, line), F32),
            pltpu.VMEM((NY, 4, own, line), F32),
            pltpu.VMEM((2, NY, 1, line), F32),
            pltpu.VMEM(state.shape, F32),
            pltpu.VMEM((2816, 128), F32),
            pltpu.SemaphoreType.DMA((SENDS,)),
            pltpu.SemaphoreType.DMA((COPIES,)),
            pltpu.SemaphoreType.DMA((STRAIGHT,)),
            pltpu.SemaphoreType.DMA((5,)),
        ],
        compiler_params=pltpu.CompilerParams(
            collective_id=0, has_side_effects=True, vmem_limit_bytes=VMEM_BYTES),
    )(
        state, member_level, level_weight, obs_row, state_coords, weights,
    )


def solution(mesh):
    return jax.shard_map(
        on_device,
        mesh=mesh,
        in_specs=(P("rows", "mem"), P("mem"), P(), P(), P(), P("rows", "mem")),
        out_specs=P("rows", "mem"),
        check_vma=False,
    )
```
